32 devices in a mesh: grp: 2 (over x), row: 16 (over z, y, core).
Axes of the slice: x: 2, y: 2, z: 4, core: 2. Of those that a mesh axis runs over, the one named last changes fastest.
Arguments:
- sequence_features: bfloat16 [256, 128, 64], P('grp', 'row'), parts along dimension 0, may hold values from -6 to 6
- edge_features: bfloat16 [256, 128, 128], P(('grp', 'row')), parts along dimension 0, may hold values from -6 to 6
- residue_features: bfloat16 [256, 384], P(('grp', 'row')), parts along dimension 0, may hold values from -6 to 6
- polymer_labels: int32 [256], P('grp'), parts along dimension 0, may hold values from 0 to 7, never falling along the last dimension, each value on 1 to 64 neighbouring positions
- polymer_membership: int32 [16, 128], P('grp'), parts along dimension 0, may hold values from 0 to 1, as said below
- present_residue_flags: int32 [256], P('grp'), parts along dimension 0, may hold values 0 or 1
- sequence_scaling_vector: float32 [64], replicated, may hold values from 0.1 to 1.9
- first_embedding_matrix: bfloat16 [64, 32], replicated, may hold values from -0.75 to 0.75
- second_embedding_matrix: bfloat16 [64, 32], replicated, may hold values from -0.75 to 0.75
- contraction_matrix: bfloat16 [1024, 128], replicated, may hold values from -0.375 to 0.375
- contraction_offset: float32 [128], replicated, may hold values from -3 to 3
- feedforward_scaling_vector: float32 [128], replicated, may hold values from 0.1 to 1.9
- feedforward_switch_matrix: bfloat16 [128, 512], replicated, may hold values from -0.5 to 0.5
- widening_matrix: bfloat16 [128, 512], replicated, may hold values from -0.5 to 0.5
- narrowing_matrix: bfloat16 [512, 128], replicated, may hold values from -0.25 to 0.25
- logit_scaling_vector: float32 [128], replicated, may hold values from 0.1 to 1.9
- edge_logit_matrix: bfloat16 [128, 16], replicated, may hold values from -2 to 2
- residue_scaling_vector: float32 [384], replicated, may hold values from 0.1 to 1.9
- asking_matrix: bfloat16 [384, 384], replicated, as said below
- lookup_matrix: bfloat16 [384, 384], replicated, as said below
- content_matrix: bfloat16 [384, 384], replicated, may hold values from -0.3125 to 0.3125
- heads_sigmoid_matrix: bfloat16 [384, 384], replicated, may hold values from -0.3125 to 0.3125
- heads_merge_matrix: bfloat16 [384, 384], replicated, may hold values from -0.3125 to 0.3125
Outputs:
- pair_out: bfloat16 [256, 128, 128], P(('grp', 'row')), parts along dimension 0
- single_out: bfloat16 [256, 384], P(('grp', 'row')), parts along dimension 0
The draws below stay inside these ranges and needn't reach their ends.
There are 2 independent parts, one for each index of `grp`. The reference program is written for one: setup_inputs(seed, part) draws one part's arguments, and reference() takes and returns one part's arrays. A program takes and returns all parts, laid end to end along the dimension named above; an argument that names none is the same for every part. Nothing has to cross between parts.
Inputs may be any that keep to these rules, and one draw needn't show every extreme that they name: `polymer_labels`: never falling along the tokens. `polymer_membership`: entry [c, s] is 1 where chain c takes part in MSA row s; every chain takes part in exactly 64 rows. `present_residue_flags`: 1 marks a real token. `asking_matrix`: a real matrix. `lookup_matrix`: a real matrix.
All inputs are finite; a program needn't handle non-finite values.
Results may differ from the reference program's by a relative error of at most 0.012.
Values may be sent and summed in bfloat16 or wider, within the bound.
No kernel may reach another device: no remote copies, remote signals or barrier semaphores. Data moves between devices by JAX's collectives and lax.ppermute only.
A program may use at most 128 MiB of HBM per device.

```python
import math
import jax
import jax.numpy as jnp
import numpy as np
from jax import lax

SEQUENCE_DEPTH = 64
FEATURE_SIZE = 32
CZ = 128
HID = 512
CS = 384
HEADS = 16
SEQUENCE_TOTAL = 128
CHAINS = 8
RESIDUE_TOTAL = 128
HEAD_DIM = 24


def projection_pair(key):
    offset_begin = jax.random.fold_in(key, 7301)
    first, second = jax.random.split(offset_begin)
    scaled = jnp.sqrt(jnp.float32(CS))
    keys = jax.random.normal(first, (CS, CS), jnp.float32) / scaled
    queries = jax.random.normal(second, (CS, CS), jnp.float32) / scaled
    return (queries, keys)


def draw_asking_matrix(key, part):
    return projection_pair(key)[0].astype(jnp.bfloat16)


def draw_lookup_matrix(key, part):
    return projection_pair(key)[1].astype(jnp.bfloat16)


def draw_polymer_membership(key, part):
    offset_begin = jax.random.fold_in(key, 4409)
    participants = []
    for polymer in range(CHAINS - 1):
        sorting_permutation = jax.random.permutation(jax.random.fold_in(offset_begin, polymer), SEQUENCE_TOTAL)
        position = jnp.argsort(sorting_permutation)
        participants.append((position < SEQUENCE_TOTAL // 2).astype(jnp.int32))
    participants.append(1 - participants[0])
    return jnp.stack(participants, axis=0).astype(jnp.int32)


def set_ends(values, stream_key, least, top_value):
    shape = values.shape
    index_at = [jax.random.randint(jax.random.fold_in(stream_key, axis), (), 0, shape[axis]) for axis in range(len(shape))]
    values = values.at[tuple(index_at)].set(least)
    longest = shape.index(max(shape))
    index_at[longest] = (index_at[longest] + 1) % shape[longest]
    return values.at[tuple(index_at)].set(top_value)


def block_scale(key, extent, pieces, least, high):
    factor_of, own = 1.0, jax.random.fold_in(key, 6)
    for dim, blocks in pieces:
        steps = jnp.exp(jax.random.uniform(jax.random.fold_in(own, dim), (blocks,), jnp.float32, least / len(pieces), high / len(pieces)))
        factor_of = factor_of * jnp.repeat(steps, extent[dim] // blocks).reshape([-1 if axis == dim else 1 for axis in range(len(extent))])
    return factor_of


def length_profile(amount, total, reach, slope):
    portions = [(1 << 20) // math.isqrt(rank ** slope) + 1 for rank in range(2, amount + 1)]
    surplus, holding = total - reach - (amount - 1), [1] * (amount - 1)
    while surplus > 0:
        candidates = [i for i in range(amount - 1) if holding[i] < reach]
        pool, budget = sum([portions[i] for i in candidates]), surplus
        for i in candidates:
            more = min(reach - holding[i], max(1, budget * portions[i] // pool), surplus)
            holding[i] = holding[i] + more
            surplus = surplus - more
    return np.array([reach] + holding)


def ragged(rng, amount, total, bound, lean):
    if amount == 2:
        one = jax.random.randint(rng, (), max(1, total - bound), min(bound, total - 1) + 1)
        return jnp.stack([one, total - one])
    lengths = jnp.asarray(length_profile(amount, total, bound, lean), jnp.int32)
    twos = (amount - 1) // 2
    giver, receiver = lengths[1:1 + 2 * twos:2], lengths[2:2 + 2 * twos:2]
    margin = jnp.minimum(giver - 1, bound - receiver)
    moved = jax.random.randint(jax.random.fold_in(rng, 1), (twos,), 0, 1 << 20) % (margin + 1)
    lengths = lengths.at[1:1 + 2 * twos:2].set(giver - moved).at[2:2 + 2 * twos:2].set(receiver + moved)
    return lengths[jax.random.permutation(jax.random.fold_in(rng, 2), amount)]


def gaussian(stream_key, dims, scale, most, shards=(), kind=jnp.bfloat16):
    level = block_scale(stream_key, dims, shards, -0.22, 0.18) if shards else 1.0
    drawn = jax.random.normal(stream_key, dims, jnp.float32) * scale * level
    return jnp.minimum(jnp.maximum(drawn, -most), most).astype(kind)


def setup_inputs(seed: int = 0, part: int = 0) -> dict:
    arg_keys = jax.random.split(jax.random.key(seed), 24)
    part_splits = jax.random.split(jax.random.fold_in(arg_keys[23], part), 24)
    sequence_features = gaussian(part_splits[0], (SEQUENCE_TOTAL, RESIDUE_TOTAL, SEQUENCE_DEPTH), 1.0, 6.0, ((1, 16),))
    edge_features = gaussian(part_splits[1], (RESIDUE_TOTAL, RESIDUE_TOTAL, CZ), 1.0, 6.0, ((0, 16),))
    residue_features = gaussian(part_splits[2], (RESIDUE_TOTAL, CS), 1.0, 6.0, ((0, 16),))
    polymer_labels = jnp.searchsorted(jnp.cumsum(ragged(part_splits[3], CHAINS, RESIDUE_TOTAL, RESIDUE_TOTAL // 2, 2)), jnp.arange(RESIDUE_TOTAL), side="right").astype(jnp.int32)
    polymer_membership = draw_polymer_membership(jax.random.fold_in(jax.random.fold_in(arg_keys[23], part), 71), part)
    present_residue_flags = set_ends((jax.random.randint(part_splits[5], (RESIDUE_TOTAL,), 0, 8) < 7).astype(jnp.int32), jax.random.fold_in(part_splits[5], 1), 0, 1)
    sequence_scaling_vector = jnp.clip(1.0 + 0.18 * jax.random.normal(arg_keys[6], (SEQUENCE_DEPTH,), jnp.float32), 0.1, 1.9)
    first_embedding_matrix = gaussian(arg_keys[7], (SEQUENCE_DEPTH, FEATURE_SIZE), SEQUENCE_DEPTH ** -0.5, 0.75)
    second_embedding_matrix = gaussian(arg_keys[8], (SEQUENCE_DEPTH, FEATURE_SIZE), SEQUENCE_DEPTH ** -0.5, 0.75)
    contraction_matrix = gaussian(arg_keys[9], (FEATURE_SIZE * FEATURE_SIZE, CZ), (FEATURE_SIZE * FEATURE_SIZE // 4) ** -0.5, 0.375)
    contraction_offset = gaussian(arg_keys[10], (CZ,), 0.5, 3.0, (), jnp.float32)
    feedforward_scaling_vector = jnp.clip(1.0 + 0.18 * jax.random.normal(arg_keys[11], (CZ,), jnp.float32), 0.1, 1.9)
    feedforward_switch_matrix = gaussian(arg_keys[12], (CZ, HID), CZ ** -0.5, 0.5)
    widening_matrix = gaussian(arg_keys[13], (CZ, HID), CZ ** -0.5, 0.5)
    narrowing_matrix = gaussian(arg_keys[14], (HID, CZ), HID ** -0.5, 0.25)
    logit_scaling_vector = jnp.clip(1.0 + 0.18 * jax.random.normal(arg_keys[15], (CZ,), jnp.float32), 0.1, 1.9)
    edge_logit_matrix = gaussian(arg_keys[16], (CZ, HEADS), (CZ // 16) ** -0.5, 2.0)
    residue_scaling_vector = jnp.clip(1.0 + 0.18 * jax.random.normal(arg_keys[17], (CS,), jnp.float32), 0.1, 1.9)
    asking_matrix = draw_asking_matrix(jax.random.fold_in(arg_keys[23], 71), part)
    lookup_matrix = draw_lookup_matrix(jax.random.fold_in(arg_keys[23], 71), part)
    content_matrix = gaussian(arg_keys[20], (CS, CS), CS ** -0.5, 0.3125)
    heads_sigmoid_matrix = gaussian(arg_keys[21], (CS, CS), CS ** -0.5, 0.3125)
    heads_merge_matrix = gaussian(arg_keys[22], (CS, CS), CS ** -0.5, 0.3125)
    return {"sequence_features": sequence_features, "edge_features": edge_features, "residue_features": residue_features, "polymer_labels": polymer_labels, "polymer_membership": polymer_membership, "present_residue_flags": present_residue_flags, "sequence_scaling_vector": sequence_scaling_vector, "first_embedding_matrix": first_embedding_matrix, "second_embedding_matrix": second_embedding_matrix, "contraction_matrix": contraction_matrix, "contraction_offset": contraction_offset, "feedforward_scaling_vector": feedforward_scaling_vector, "feedforward_switch_matrix": feedforward_switch_matrix, "widening_matrix": widening_matrix, "narrowing_matrix": narrowing_matrix, "logit_scaling_vector": logit_scaling_vector, "edge_logit_matrix": edge_logit_matrix, "residue_scaling_vector": residue_scaling_vector, "asking_matrix": asking_matrix, "lookup_matrix": lookup_matrix, "content_matrix": content_matrix, "heads_sigmoid_matrix": heads_sigmoid_matrix, "heads_merge_matrix": heads_merge_matrix}


epsilon = 1e-05
highest = lax.Precision.HIGHEST

def standardize_features(values, scales):
    values = values.astype(jnp.float32)
    centred = values - lax.optimization_barrier(jnp.mean(values, axis=-1, keepdims=True))
    spread = lax.optimization_barrier(jnp.mean(centred * centred, axis=-1, keepdims=True))
    return centred * lax.rsqrt(spread + epsilon) * scales

def reference(sequence_features, edge_features, residue_features, polymer_labels, polymer_membership, present_residue_flags, sequence_scaling_vector, first_embedding_matrix, second_embedding_matrix, contraction_matrix, contraction_offset, feedforward_scaling_vector, feedforward_switch_matrix, widening_matrix, narrowing_matrix, logit_scaling_vector, edge_logit_matrix, residue_scaling_vector, asking_matrix, lookup_matrix, content_matrix, heads_sigmoid_matrix, heads_merge_matrix):
    onehot = (polymer_labels[:, None] == jnp.arange(CHAINS, dtype=jnp.int32)[None, :]).astype(jnp.float32)
    pair_rows = polymer_membership.astype(jnp.float32)
    sequence_present_flags = jnp.dot(onehot, pair_rows, precision=highest).T
    shared = jnp.dot(pair_rows, pair_rows.T, precision=highest)
    counts = jnp.dot(jnp.dot(onehot, shared, precision=highest), onehot.T, precision=highest)
    standardized_sequences = standardize_features(sequence_features, sequence_scaling_vector).astype(jnp.bfloat16).reshape(SEQUENCE_TOTAL * RESIDUE_TOTAL, SEQUENCE_DEPTH)
    first_embedding_entries = (jnp.dot(standardized_sequences, first_embedding_matrix, preferred_element_type=jnp.float32).reshape(SEQUENCE_TOTAL, RESIDUE_TOTAL, FEATURE_SIZE) * sequence_present_flags[:, :, None]).astype(jnp.bfloat16)
    second_embedding_entries = (jnp.dot(standardized_sequences, second_embedding_matrix, preferred_element_type=jnp.float32).reshape(SEQUENCE_TOTAL, RESIDUE_TOTAL, FEATURE_SIZE) * sequence_present_flags[:, :, None]).astype(jnp.bfloat16)
    second_merged = second_embedding_entries.reshape(SEQUENCE_TOTAL, RESIDUE_TOTAL * FEATURE_SIZE)
    sequence_group = min(16, RESIDUE_TOTAL)

    def pair_block(beginning):
        first_sequences = lax.dynamic_slice_in_dim(first_embedding_entries, beginning, sequence_group, 1).reshape(SEQUENCE_TOTAL, sequence_group * FEATURE_SIZE)
        outer = lax.dot_general(first_sequences, second_merged, (((0,), (0,)), ((), ())), preferred_element_type=jnp.float32)
        outer = outer.reshape(sequence_group, FEATURE_SIZE, RESIDUE_TOTAL, FEATURE_SIZE).transpose(0, 2, 1, 3).reshape(sequence_group, RESIDUE_TOTAL, FEATURE_SIZE * FEATURE_SIZE)
        shared_rows = lax.dynamic_slice_in_dim(counts, beginning, sequence_group, 0)
        outer = (outer / jnp.maximum(shared_rows, 1.0)[:, :, None]).astype(jnp.bfloat16)
        update = jnp.dot(outer.reshape(sequence_group * RESIDUE_TOTAL, FEATURE_SIZE * FEATURE_SIZE), contraction_matrix, preferred_element_type=jnp.float32) + contraction_offset
        old_rows = lax.dynamic_slice_in_dim(edge_features, beginning, sequence_group, 0).reshape(sequence_group * RESIDUE_TOTAL, CZ)
        pair_one = (old_rows.astype(jnp.float32) + update).astype(jnp.bfloat16)
        normed_pair = standardize_features(pair_one, feedforward_scaling_vector).astype(jnp.bfloat16)
        gated = jnp.dot(normed_pair, feedforward_switch_matrix, preferred_element_type=jnp.float32)
        lifted = jnp.dot(normed_pair, widening_matrix, preferred_element_type=jnp.float32)
        hidden = (jax.nn.silu(gated) * lifted).astype(jnp.bfloat16)
        pair_two = (pair_one.astype(jnp.float32) + jnp.dot(hidden, narrowing_matrix, preferred_element_type=jnp.float32)).astype(jnp.bfloat16)
        bias_normed = standardize_features(pair_two, logit_scaling_vector).astype(jnp.bfloat16)
        bias_rows = jnp.dot(bias_normed, edge_logit_matrix, preferred_element_type=jnp.float32)
        return (pair_two.reshape(sequence_group, RESIDUE_TOTAL, CZ), bias_rows.reshape(sequence_group, RESIDUE_TOTAL, HEADS))
    starts = jnp.arange(0, RESIDUE_TOTAL, sequence_group, dtype=jnp.int32)
    pair_out, bias_all = lax.map(pair_block, starts)
    pair_out = pair_out.reshape(RESIDUE_TOTAL, RESIDUE_TOTAL, CZ)
    bias_all = bias_all.reshape(RESIDUE_TOTAL, RESIDUE_TOTAL, HEADS)
    normed_single = standardize_features(residue_features, residue_scaling_vector).astype(jnp.bfloat16)
    query = jnp.dot(normed_single, asking_matrix, preferred_element_type=jnp.float32).astype(jnp.bfloat16)
    keys = jnp.dot(normed_single, lookup_matrix, preferred_element_type=jnp.float32).astype(jnp.bfloat16)
    values = jnp.dot(normed_single, content_matrix, preferred_element_type=jnp.float32).astype(jnp.bfloat16)
    sigmoid_gate = jax.nn.sigmoid(jnp.dot(normed_single, heads_sigmoid_matrix, preferred_element_type=jnp.float32))
    query_heads = query.astype(jnp.float32).reshape(RESIDUE_TOTAL, HEADS, HEAD_DIM)
    key_heads = keys.astype(jnp.float32).reshape(RESIDUE_TOTAL, HEADS, HEAD_DIM)
    value_heads = values.astype(jnp.float32).reshape(RESIDUE_TOTAL, HEADS, HEAD_DIM)
    scores = jnp.einsum('ihd,jhd->hij', query_heads, key_heads) / math.sqrt(HEAD_DIM) + bias_all.transpose(2, 0, 1)
    live = (present_residue_flags == 1)[None, None, :]
    scores = jnp.where(live, scores, -1e+30)
    peaks = lax.optimization_barrier(jnp.max(scores, axis=-1, keepdims=True))
    expos = jnp.where(live, jnp.exp(scores - peaks), 0.0)
    totals = lax.optimization_barrier(jnp.sum(expos, axis=-1))
    weights = expos.astype(jnp.bfloat16)
    mixed = jnp.einsum('hij,jhd->ihd', weights.astype(jnp.float32), value_heads) / totals.T[:, :, None]
    attended = (mixed.reshape(RESIDUE_TOTAL, CS) * sigmoid_gate).astype(jnp.bfloat16)
    single_out = (residue_features.astype(jnp.float32) + jnp.dot(attended, heads_merge_matrix, preferred_element_type=jnp.float32)).astype(jnp.bfloat16)
    return (pair_out, single_out)
```

```python
import math

import jax
import jax.numpy as jnp
from jax import lax
from jax.experimental import pallas as pl
from jax.experimental.pallas import tpu as pltpu
from jax.sharding import PartitionSpec as P

epsilon = 1e-05
highest = lax.Precision.HIGHEST
f32 = jnp.float32
bf16 = jnp.bfloat16
LANES = 128


def standardize_features(values, scales):
    values = values.astype(jnp.float32)
    centred = values - jnp.mean(values, axis=-1, keepdims=True)
    spread = jnp.mean(centred * centred, axis=-1, keepdims=True)
    return centred * lax.rsqrt(spread + epsilon) * scales


def general(
    sequence_features,
    edge_features,
    residue_features,
    polymer_labels,
    polymer_membership,
    present_residue_flags,
    sequence_scaling_vector,
    first_embedding_matrix,
    second_embedding_matrix,
    contraction_matrix,
    contraction_offset,
    feedforward_scaling_vector,
    feedforward_switch_matrix,
    widening_matrix,
    narrowing_matrix,
    logit_scaling_vector,
    edge_logit_matrix,
    residue_scaling_vector,
    asking_matrix,
    lookup_matrix,
    content_matrix,
    heads_sigmoid_matrix,
    heads_merge_matrix,
):
    token_row_count = residue_features.shape[0]
    sequence_entries = sequence_features.shape[0]
    sequence_depth = sequence_features.shape[2]
    factor_channels_width = first_embedding_matrix.shape[1]
    pair_width = edge_features.shape[2]
    all_tokens = edge_features.shape[1]
    chains = polymer_membership.shape[0]
    heads = edge_logit_matrix.shape[1]
    single_width = residue_features.shape[1]
    head_size = single_width // heads
    first_token = lax.axis_index("row") * token_row_count
    onehot_all = (polymer_labels[:, None] == jnp.arange(chains, dtype=jnp.int32)[None, :]).astype(
        jnp.float32
    )
    onehot_mine = lax.dynamic_slice_in_dim(onehot_all, first_token, token_row_count, 0)
    pair_rows = polymer_membership.astype(jnp.float32)
    sequence_present_flags = jnp.dot(onehot_mine, pair_rows, precision=highest).T
    shared = jnp.dot(pair_rows, pair_rows.T, precision=highest)
    counts = jnp.dot(
        jnp.dot(onehot_mine, shared, precision=highest), onehot_all.T, precision=highest
    )
    standardized_sequences = standardize_features(
        sequence_features, sequence_scaling_vector
    ).astype(jnp.bfloat16)
    flattened_alignment = standardized_sequences.reshape(
        sequence_entries * token_row_count, sequence_depth
    )
    first_embedding_entries = (
        jnp.dot(
            flattened_alignment, first_embedding_matrix, preferred_element_type=jnp.float32
        ).reshape(sequence_entries, token_row_count, factor_channels_width)
        * sequence_present_flags[:, :, None]
    ).astype(jnp.bfloat16)
    left_flattened = first_embedding_entries.reshape(
        sequence_entries, token_row_count * factor_channels_width
    )
    second_embedding_entries = (
        jnp.dot(
            flattened_alignment, second_embedding_matrix, preferred_element_type=jnp.float32
        ).reshape(sequence_entries, token_row_count, factor_channels_width)
        * sequence_present_flags[:, :, None]
    ).astype(jnp.bfloat16)

    def finish_block(outer, column_start, stride_columns):
        shared_cols = lax.dynamic_slice_in_dim(counts, column_start, stride_columns, 1)
        outer = (outer / jnp.maximum(shared_cols, 1.0)[:, :, None]).astype(jnp.bfloat16)
        update = (
            jnp.dot(
                outer.reshape(
                    token_row_count * stride_columns, factor_channels_width * factor_channels_width
                ),
                contraction_matrix,
                preferred_element_type=jnp.float32,
            )
            + contraction_offset
        )
        old_cols = lax.dynamic_slice_in_dim(edge_features, column_start, stride_columns, 1).reshape(
            token_row_count * stride_columns, pair_width
        )
        return (
            (old_cols.astype(jnp.float32) + update)
            .astype(jnp.bfloat16)
            .reshape(token_row_count, stride_columns, pair_width)
        )

    factor_piece = lax.all_gather(second_embedding_entries, "row", axis=1, tiled=True)
    width = factor_piece.shape[1]
    stride_columns = math.gcd(width, 128)

    def one_block(offset):
        panel = lax.dynamic_slice_in_dim(factor_piece, offset, stride_columns, 1).reshape(
            sequence_entries, stride_columns * factor_channels_width
        )
        outer = lax.dot_general(
            left_flattened, panel, (((0,), (0,)), ((), ())), preferred_element_type=jnp.float32
        )
        outer = outer.reshape(
            token_row_count, factor_channels_width, stride_columns, factor_channels_width
        ).transpose(0, 2, 1, 3)
        outer = outer.reshape(
            token_row_count, stride_columns, factor_channels_width * factor_channels_width
        )
        return finish_block(outer, offset, stride_columns)

    blocks = lax.map(one_block, jnp.arange(0, width, stride_columns, dtype=jnp.int32))
    pair_one = blocks.transpose(1, 0, 2, 3).reshape(token_row_count, width, pair_width)
    flat_pair = pair_one.reshape(token_row_count * all_tokens, pair_width)
    normed_pair = standardize_features(flat_pair, feedforward_scaling_vector).astype(jnp.bfloat16)
    gated = jnp.dot(normed_pair, feedforward_switch_matrix, preferred_element_type=jnp.float32)
    lifted = jnp.dot(normed_pair, widening_matrix, preferred_element_type=jnp.float32)
    hidden = (jax.nn.silu(gated) * lifted).astype(jnp.bfloat16)
    pair_two = (
        flat_pair.astype(jnp.float32)
        + jnp.dot(hidden, narrowing_matrix, preferred_element_type=jnp.float32)
    ).astype(jnp.bfloat16)
    bias_normed = standardize_features(pair_two, logit_scaling_vector).astype(jnp.bfloat16)
    bias_rows = jnp.dot(bias_normed, edge_logit_matrix, preferred_element_type=jnp.float32)
    bias_heads = bias_rows.reshape(token_row_count, all_tokens, heads).transpose(2, 0, 1)
    pair_out = pair_two.reshape(token_row_count, all_tokens, pair_width)
    normed_single = standardize_features(residue_features, residue_scaling_vector).astype(
        jnp.bfloat16
    )
    query = jnp.dot(normed_single, asking_matrix, preferred_element_type=jnp.float32).astype(
        jnp.bfloat16
    )
    query_heads = query.reshape(token_row_count, heads, head_size)
    sigmoid_gate = jax.nn.sigmoid(
        jnp.dot(normed_single, heads_sigmoid_matrix, preferred_element_type=jnp.float32)
    )
    scale = 1.0 / math.sqrt(head_size)
    piece = lax.all_gather(normed_single, "row", axis=0, tiled=True)
    keys_piece = jnp.dot(piece, lookup_matrix, preferred_element_type=jnp.float32).astype(
        jnp.bfloat16
    )
    values_piece = jnp.dot(piece, content_matrix, preferred_element_type=jnp.float32).astype(
        jnp.bfloat16
    )
    width = keys_piece.shape[0]
    key_heads = keys_piece.reshape(width, heads, head_size)
    value_heads = values_piece.reshape(width, heads, head_size)
    scores = (
        jnp.einsum("ihd,jhd->hij", query_heads, key_heads, preferred_element_type=jnp.float32)
        * scale
    )
    scores = scores + bias_heads
    live = (present_residue_flags == 1)[None, None, :]
    scores = jnp.where(live, scores, -1e30)
    peak_old = jnp.full((heads, token_row_count), -1e30, jnp.float32)
    peak_new = jnp.maximum(peak_old, jnp.max(scores, axis=-1))
    expos = jnp.where(live, jnp.exp(scores - peak_new[:, :, None]), 0.0)
    total_new = jnp.sum(expos, axis=-1)
    accum_new = jnp.einsum(
        "hij,jhd->hid", expos.astype(jnp.bfloat16), value_heads, preferred_element_type=jnp.float32
    )
    mixed = accum_new / total_new[:, :, None]
    mixed = mixed.transpose(1, 0, 2).reshape(token_row_count, single_width)
    attended = (mixed * sigmoid_gate).astype(jnp.bfloat16)
    single_out = (
        residue_features.astype(jnp.float32)
        + jnp.dot(attended, heads_merge_matrix, preferred_element_type=jnp.float32)
    ).astype(jnp.bfloat16)
    return (pair_out, single_out)


def dot_nt(a, b):
    return lax.dot_general(a, b, (((1,), (1,)), ((), ())), preferred_element_type=f32)


def dot(a, b):
    return jnp.dot(a, b, preferred_element_type=f32)


def iota(shape, dim):
    return lax.broadcasted_iota(jnp.int32, shape, dim)


def row_ranks(member):
    rows = member.shape[1]
    upto = (iota((rows, rows), 0) <= iota((rows, rows), 1)).astype(bf16)
    return dot(member.astype(bf16), upto) * member


def pick_rows(ranks, kept):
    return (ranks == (iota((kept, ranks.shape[1]), 0) + 1).astype(f32)).astype(bf16)


def message_kernel(
    labels, sequence, member, second_t, gain, residue, residue_gain, out, raw, ranks, factor
):
    rows, tokens, _ = sequence.shape
    width = second_t.shape[0]
    kept = rows // 2
    first = lax.axis_index("row") * tokens
    raw[...] = sequence[...].astype(f32).reshape(raw.shape)
    ranks[...] = row_ranks(member[...].astype(f32))
    for t in range(tokens):
        chosen = pick_rows(ranks[pl.ds(labels[first + t], 1), :], kept)
        live = dot(chosen, raw[pl.ds(t, rows, stride=tokens), :].astype(bf16))
        normed = standardize_features(live, gain[...]).astype(bf16)
        normed = jnp.concatenate([normed, normed], 0)
        factor[t * width : (t + 1) * width, :] = dot_nt(second_t[...], normed)
    low = iota((tokens, 2 * kept), 1) < kept
    for d in range(0, width, 2):
        even = factor[pl.ds(d, tokens, stride=width), :]
        odd = factor[pl.ds(d + 1, tokens, stride=width), :]
        out[:, d * kept : (d + 2) * kept] = jnp.where(low, even, odd).astype(bf16)
    out[:, width * kept :] = standardize_features(residue[...], residue_gain[...]).astype(bf16)


def local_kernel(
    labels,
    label_row,
    sequence,
    member,
    first_t,
    gain,
    residue,
    residue_gain,
    asking,
    gating,
    edges,
    offset,
    pair_gain,
    logit_gain,
    contraction,
    switch,
    widening,
    narrowing,
    edge_logit,
    left_out,
    query_out,
    gate_out,
    base_out,
    scale_out,
    pair_gain_out,
    logit_gain_out,
    contraction_out,
    up_out,
    down_out,
    logit_out,
    normed,
    ranks,
    shared,
    factors,
    planes,
):
    rows, tokens, features = sequence.shape
    width = first_t.shape[0]
    chains = member.shape[0]
    kept = rows // 2
    heads = edge_logit.shape[1]
    size = residue.shape[1] // heads
    first = lax.axis_index("row") * tokens
    members = member[...].astype(f32)
    ranks[...] = row_ranks(members)
    onehot = (iota((chains, label_row.shape[1]), 0) == label_row[...]).astype(bf16)
    overlap = dot_nt(members.astype(bf16), members.astype(bf16))
    shared[...] = 1.0 / jnp.maximum(dot(overlap.astype(bf16), onehot), 1.0)
    wide = sequence[...].astype(f32).reshape(rows * tokens, features)
    normed[...] = standardize_features(wide, gain[...]).astype(bf16).astype(f32)
    for t in range(tokens):
        chain = labels[first + t]
        mine = normed[pl.ds(t, rows, stride=tokens), :].astype(bf16)
        present = (ranks[pl.ds(chain, 1), :] > 0.0).astype(f32)
        factors[t * width : (t + 1) * width, :] = (dot_nt(first_t[...], mine) * present).astype(bf16)
        scale_out[t : t + 1, :] = shared[pl.ds(chain, 1), :]
    for c in range(chains):
        chosen = pick_rows(ranks[c : c + 1, :], kept)
        planes[c * kept : (c + 1) * kept, :] = chosen
    left_out[...] = dot_nt(factors[...], planes[...]).astype(bf16)

    normed_single = standardize_features(residue[...], residue_gain[...]).astype(bf16)
    query = dot(normed_single, asking[...]).astype(bf16).astype(f32)
    lane = iota((heads, heads * size), 1)
    low = iota((heads, heads * size), 0) * size
    own = jnp.logical_and(lane >= low, lane < low + size)
    for t in range(tokens):
        spread = jnp.where(own, jnp.broadcast_to(query[t : t + 1, :], own.shape), 0.0)
        query_out[t * heads : (t + 1) * heads, :] = spread.astype(bf16)
    gate_out[...] = jax.nn.sigmoid(dot(normed_single, gating[...]))

    channels = offset.shape[1]
    square = (channels, channels)
    offset_t = jnp.broadcast_to(offset[...], square).T
    pair_gain_out[...] = jnp.broadcast_to(pair_gain[...], square).T
    logit_gain_out[...] = jnp.broadcast_to(logit_gain[...], square).T
    for t in range(tokens):
        base_out[t] = edges[t].astype(f32).T + offset_t
    hidden = switch.shape[1]
    for k in range(0, hidden, channels):
        up_out[k : k + channels, :] = switch[:, k : k + channels].astype(f32).T.astype(bf16)
        up_out[hidden + k : hidden + k + channels, :] = (
            widening[:, k : k + channels].astype(f32).T.astype(bf16)
        )
        down_out[:, k : k + channels] = narrowing[k : k + channels, :].astype(f32).T.astype(bf16)
    padded = jnp.concatenate(
        [edge_logit[...].astype(f32), jnp.zeros((channels, channels - heads), f32)], 1
    )
    logit_out[...] = padded.T[:heads].astype(bf16)


def finish_kernel(
    here_own,
    here_core,
    there_own,
    there_core,
    label_row,
    live_row,
    left,
    query,
    gate,
    base,
    scale,
    pair_gain,
    logit_gain,
    contraction_t,
    up_t,
    down_t,
    logit_t,
    lookup,
    content,
    merge,
    residue,
    pair_out,
    single_out,
    gathered,
    outer,
    bias,
    *,
    slots,
):
    tokens, channels, columns = base.shape
    single = residue.shape[1]
    heads = logit_t.shape[0]
    chains, kept, width = slots["chains"], slots["kept"], slots["width"]
    me = lax.axis_index("row")
    for array, marks in (
        (here_own, slots["here_own"]),
        (here_core, slots["here_core"]),
        (there_own, slots["there_own"]),
        (there_core, slots["there_core"]),
    ):
        for n, mark in enumerate(marks):
            gathered[me ^ mark] = array[n]

    chain_of = label_row[...]
    inside = [
        jnp.broadcast_to((chain_of == c).astype(bf16), (kept, columns)) for c in range(chains)
    ]
    for d in range(0, width, 2):
        block = gathered[:, :, d * kept : (d + 2) * kept].astype(f32).reshape(columns, 2 * kept)
        flipped = block.T.astype(bf16)
        right = jnp.concatenate(
            [
                jnp.concatenate([flipped[:kept] * m for m in inside], 0),
                jnp.concatenate([flipped[kept:] * m for m in inside], 0),
            ],
            1,
        )
        outer[:, d * columns : (d + 2) * columns] = dot(left[...], right).astype(bf16)

    def norm(x, gains):
        centred = x - jnp.mean(x, axis=0, keepdims=True)
        spread = jnp.mean(centred * centred, axis=0, keepdims=True)
        return (centred * lax.rsqrt(spread + epsilon) * gains).astype(bf16)

    hidden = down_t.shape[1]
    gains = jnp.concatenate([pair_gain[...]] * 2, 1)
    more_gains = jnp.concatenate([logit_gain[...]] * 2, 1)
    for i in range(0, tokens, 2):
        right = jnp.concatenate(
            [
                jnp.concatenate(
                    [
                        outer[n * width : (n + 1) * width, d * columns : (d + 1) * columns]
                        for d in range(width)
                    ],
                    0,
                )
                for n in (i, i + 1)
            ],
            1,
        )
        shrink = jnp.concatenate([scale[i : i + 1, :], scale[i + 1 : i + 2, :]], 1)
        start = jnp.concatenate([base[i], base[i + 1]], 1)
        pair_one = (start + dot(contraction_t[...], right) * shrink).astype(bf16).astype(f32)
        lifted = dot(up_t[...], norm(pair_one, gains))
        gated = lifted[:hidden]
        half = gated * 0.5
        acted = ((half + half * jnp.tanh(half)) * lifted[hidden:]).astype(bf16)
        pair_two = (pair_one + dot(down_t[...], acted)).astype(bf16).astype(f32)
        logits = dot(logit_t[...], norm(pair_two, more_gains))
        for n in range(2):
            bias[(i + n) * heads : (i + n + 1) * heads, :] = logits[:, n * columns : (n + 1) * columns]
            pair_out[i + n] = pair_two[:, n * columns : (n + 1) * columns].T.astype(bf16)

    start = width * kept
    everyone = gathered[:, :, start:].astype(f32).reshape(columns, single).astype(bf16)
    key = dot(everyone, lookup[...]).astype(bf16)
    value = dot(everyone, content[...]).astype(bf16)
    scores = dot_nt(query[...], key) * (1.0 / math.sqrt(single // heads)) + bias[...]
    live = live_row[...] == 1
    scores = jnp.where(live, scores, -1e30)
    peak = jnp.max(scores, axis=-1, keepdims=True)
    weights = jnp.where(live, jnp.exp(scores - peak), 0.0)
    total = jnp.sum(weights, axis=-1, keepdims=True)
    mixed = dot(weights.astype(bf16), value) / total
    size = single // heads
    lane = iota((heads, single), 1)
    low = iota((heads, single), 0) * size
    own = jnp.logical_and(lane >= low, lane < low + size)
    taken = [
        jnp.sum(jnp.where(own, mixed[t * heads : (t + 1) * heads], 0.0), axis=0, keepdims=True)
        for t in range(tokens)
    ]
    attended = (jnp.concatenate(taken, 0) * gate[...]).astype(bf16)
    single_out[...] = (residue[...].astype(f32) + dot(attended, merge[...])).astype(bf16)


def in_vmem(count):
    return [pl.BlockSpec(memory_space=pltpu.VMEM) for _ in range(count)]


def scalars():
    return pl.BlockSpec(memory_space=pltpu.SMEM)


def paired(step, count):
    return [(n, n ^ step) for n in range(count)]


def compact(
    sequence_features,
    edge_features,
    residue_features,
    polymer_labels,
    polymer_membership,
    present_residue_flags,
    sequence_scaling_vector,
    first_embedding_matrix,
    second_embedding_matrix,
    contraction_matrix,
    contraction_offset,
    feedforward_scaling_vector,
    feedforward_switch_matrix,
    widening_matrix,
    narrowing_matrix,
    logit_scaling_vector,
    edge_logit_matrix,
    residue_scaling_vector,
    asking_matrix,
    lookup_matrix,
    content_matrix,
    heads_sigmoid_matrix,
    heads_merge_matrix,
):
    rows, tokens, features = sequence_features.shape
    columns = edge_features.shape[1]
    channels = edge_features.shape[2]
    width = first_embedding_matrix.shape[1]
    chains = polymer_membership.shape[0]
    single = residue_features.shape[1]
    hidden = narrowing_matrix.shape[0]
    heads = edge_logit_matrix.shape[1]
    devices = columns // tokens
    kept = rows // 2
    payload = width * kept + single
    row = lambda v: v.reshape(1, -1)
    label_row = row(polymer_labels)

    message = pl.pallas_call(
        message_kernel,
        out_shape=jax.ShapeDtypeStruct((tokens, payload), bf16),
        in_specs=[scalars()] + in_vmem(6),
        out_specs=pl.BlockSpec(memory_space=pltpu.VMEM),
        scratch_shapes=[
            pltpu.VMEM((rows * tokens, features), f32),
            pltpu.VMEM((chains, rows), f32),
            pltpu.VMEM((tokens * width, 2 * kept), f32),
        ],
        name="message",
    )(
        polymer_labels,
        sequence_features,
        polymer_membership,
        second_embedding_matrix.T,
        row(sequence_scaling_vector),
        residue_features,
        row(residue_scaling_vector),
    )
    send = lambda x, step: lax.ppermute(x, "row", paired(step, devices))
    far = [step for step in range(4, devices, 4)]
    here = jnp.stack([message] + [send(message, step) for step in far])
    there = send(here, 2)
    here_core = send(here, 1)
    there_core = send(there, 1)

    contraction_t = (
        contraction_matrix.reshape(width, width, channels)
        .transpose(2, 1, 0)
        .reshape(channels, width * width)
    )
    shapes = [
        ((tokens * width, chains * kept), bf16),
        ((tokens * heads, single), bf16),
        ((tokens, single), f32),
        ((tokens, channels, columns), f32),
        ((tokens, columns), f32),
        ((channels, channels), f32),
        ((channels, channels), f32),
        ((1, 1), f32),
        ((2 * hidden, channels), bf16),
        ((channels, hidden), bf16),
        ((heads, channels), bf16),
    ]
    outs = pl.pallas_call(
        local_kernel,
        out_shape=[jax.ShapeDtypeStruct(s, d) for s, d in shapes],
        in_specs=[scalars()] + in_vmem(18),
        out_specs=in_vmem(len(shapes)),
        scratch_shapes=[
            pltpu.VMEM((rows * tokens, features), f32),
            pltpu.VMEM((chains, rows), f32),
            pltpu.VMEM((chains, columns), f32),
            pltpu.VMEM((tokens * width, rows), bf16),
            pltpu.VMEM((chains * kept, rows), bf16),
        ],
        name="local",
    )(
        polymer_labels,
        label_row,
        sequence_features,
        polymer_membership,
        first_embedding_matrix.T,
        row(sequence_scaling_vector),
        residue_features,
        row(residue_scaling_vector),
        asking_matrix,
        heads_sigmoid_matrix,
        edge_features,
        row(contraction_offset),
        row(feedforward_scaling_vector),
        row(logit_scaling_vector),
        contraction_t,
        feedforward_switch_matrix,
        widening_matrix,
        narrowing_matrix,
        edge_logit_matrix,
    )
    left, query, gate, base, scale, pair_gain, logit_gain, _, up_t, down_t, logit_t = outs
    slots = {"chains": chains, "kept": kept, "width": width}
    for name, mark in (("here_own", 0), ("here_core", 1), ("there_own", 2), ("there_core", 3)):
        slots[name] = [mark] + [mark ^ step for step in far]

    def finish(*refs):
        finish_kernel(*refs, slots=slots)

    return pl.pallas_call(
        finish,
        out_shape=[
            jax.ShapeDtypeStruct(edge_features.shape, bf16),
            jax.ShapeDtypeStruct(residue_features.shape, bf16),
        ],
        in_specs=in_vmem(21),
        out_specs=in_vmem(2),
        scratch_shapes=[
            pltpu.VMEM((devices, tokens, payload), bf16),
            pltpu.VMEM((tokens * width, width * columns), bf16),
            pltpu.VMEM((tokens * heads, columns), f32),
        ],
        name="finish",
    )(
        here,
        here_core,
        there,
        there_core,
        label_row,
        row(present_residue_flags),
        left,
        query,
        gate,
        base,
        scale,
        pair_gain,
        logit_gain,
        contraction_t,
        up_t,
        down_t,
        logit_t,
        lookup_matrix,
        content_matrix,
        heads_merge_matrix,
        residue_features,
    )


def local(*arrays):
    sequence_features, edge_features = arrays[0], arrays[1]
    rows, tokens, _ = sequence_features.shape
    _, columns, channels = edge_features.shape
    if rows == columns == channels == LANES and columns == 16 * tokens:
        return compact(*arrays)
    return general(*arrays)


def solution(mesh):
    placed = (
        P("grp", "row", None),
        P(("grp", "row"), None, None),
        P(("grp", "row"), None),
        P("grp"),
        P("grp", None),
        P("grp"),
        P(),
        P(),
        P(),
        P(),
        P(),
        P(),
        P(),
        P(),
        P(),
        P(),
        P(),
        P(),
        P(),
        P(),
        P(),
        P(),
        P(),
    )
    return jax.shard_map(
        local,
        mesh=mesh,
        in_specs=placed,
        out_specs=(P(("grp", "row"), None, None), P(("grp", "row"), None)),
        check_vma=False,
    )
```
